128 devices in a mesh: dp: 8 (over x_hi, y), seq: 16 (over x_lo, z, core).
Axes of the slice: x: 4 (x_hi: 2, x_lo: 2; x = x_hi * 2 + x_lo), y: 4, z: 4, core: 2. Of those that a mesh axis runs over, the one named last changes fastest.
Arguments:
- inputs: bfloat16 [8, 16384, 512], P('dp', 'seq'), may hold values from -0.0007324219 to 0.0007324219
- grad_out: bfloat16 [8, 16384, 512], P('dp', 'seq'), may hold values from -6 to 6
- conv_filter: bfloat16 [16384], P('seq'), may hold values from -0.046875 to 0.046875
Outputs:
- grad_input: bfloat16 [8, 16384, 512], P('dp', 'seq')
- grad_filter: float32 [16384], P('seq')
The draws below stay inside these ranges and needn't reach their ends.
All inputs are finite; a program needn't handle non-finite values.
Results may differ from the reference program's by a relative error of at most 0.0095.
Values may be sent and summed in bfloat16 or wider, within the bound.
A program may use at most 128 MiB of HBM per device.

```python
import jax
import jax.numpy as jnp
from jax import lax

CH = 512
LEN = 16384
BATCH = 8


def levels(key, extent, pieces, least, top_value):
    loudness, own = 1.0, jax.random.fold_in(key, 6)
    for dim, blocks in pieces:
        steps = jnp.exp(jax.random.uniform(jax.random.fold_in(own, dim), (blocks,), jnp.float32, least / len(pieces), top_value / len(pieces)))
        loudness = loudness * jnp.repeat(steps, extent[dim] // blocks).reshape([-1 if axis == dim else 1 for axis in range(len(extent))])
    return loudness


def noise(key, dims, scale, bound, shards=(), held_as=jnp.bfloat16):
    level = levels(key, dims, shards, -0.22, 0.18) if shards else 1.0
    result = jax.random.normal(key, dims, jnp.float32) * scale * level
    return jnp.minimum(jnp.maximum(result, -bound), bound).astype(held_as)


def setup_inputs(seed: int = 0) -> dict:
    arg_keys = jax.random.split(jax.random.key(seed), 4)
    return {
        "inputs": noise(arg_keys[0], (BATCH, LEN, CH), (LEN * CH * BATCH) ** -0.5, 0.0007324219, ((0, 8), (1, 16))),
        "grad_out": noise(arg_keys[1], (BATCH, LEN, CH), 1.0, 6.0, ((0, 8), (1, 16))),
        "conv_filter": noise(arg_keys[2], (LEN,), LEN ** -0.5, 0.046875, ((0, 16),)),
    }


def reference(inputs, grad_out, conv_filter):
    period = 2 * LEN
    filter_spec = jnp.fft.rfft(conv_filter.astype(jnp.float32), n=period)

    def per_sequence(members):
        seq_inputs, seq_grads = members
        input_spec = jnp.fft.rfft(seq_inputs.astype(jnp.float32), n=period, axis=0)
        grad_spec = jnp.fft.rfft(seq_grads.astype(jnp.float32), n=period, axis=0)
        product = jnp.conj(filter_spec)[:, None] * grad_spec
        backward = jnp.fft.irfft(product, n=period, axis=0)[:LEN]
        filter_term = jnp.sum(grad_spec * jnp.conj(input_spec), axis=1)
        return backward.astype(jnp.bfloat16), filter_term

    grad_input, filter_terms = lax.map(per_sequence, (inputs, grad_out))
    grad_filter = jnp.fft.irfft(jnp.sum(filter_terms, axis=0), n=period)[:LEN].astype(jnp.float32)
    return grad_input, grad_filter
```

```python
import jax
import jax.numpy as jnp
from jax import lax
from jax.experimental import pallas as pl
from jax.experimental.pallas import tpu as pltpu
from jax.sharding import PartitionSpec as P

BLK = 256
LANES = 128
NT = (((1,), (1,)), ((), ()))


def full(memory=pltpu.VMEM):
    return pl.BlockSpec(memory_space=memory)


def dot(a, b):
    return jnp.dot(a, b, preferred_element_type=jnp.float32)


def split_kernel(x_ref, s_ref):
    peers, _, group, _ = s_ref.shape
    turned = jnp.transpose(x_ref[...])
    for peer in range(peers):
        s_ref[peer, 0] = turned[peer * group : (peer + 1) * group]


def split(x, peers):
    rows, channels = x.shape
    group = channels // peers
    return pl.pallas_call(
        split_kernel,
        grid=(rows // BLK,),
        in_specs=[pl.BlockSpec((BLK, channels), lambda k: (k, 0))],
        out_specs=pl.BlockSpec((peers, 1, group, BLK), lambda k: (0, k, 0, 0)),
        out_shape=jax.ShapeDtypeStruct((peers, rows // BLK, group, BLK), x.dtype),
        name="split",
    )(x)


def join_kernel(s_ref, x_ref):
    peers, _, group, _ = s_ref.shape
    x_ref[...] = jnp.transpose(s_ref[...].reshape(peers * group, BLK))


def join(s):
    peers, blocks, group, _ = s.shape
    return pl.pallas_call(
        join_kernel,
        grid=(blocks,),
        in_specs=[pl.BlockSpec((peers, 1, group, BLK), lambda k: (0, k, 0, 0))],
        out_specs=pl.BlockSpec((BLK, peers * group), lambda k: (k, 0)),
        out_shape=jax.ShapeDtypeStruct((blocks * BLK, peers * group), s.dtype),
        name="join",
    )(s)


def flip_matrix(size, dtype):
    row = lax.broadcasted_iota(jnp.int32, (size, size), 0)
    col = lax.broadcasted_iota(jnp.int32, (size, size), 1)
    return jnp.where(row + col == size - 1, 1.0, 0.0).astype(dtype)


def build_strip(h_ref, turned_ref, strip_ref):
    count = h_ref.shape[0]
    turned_ref[...] = dot(h_ref[...], flip_matrix(LANES, h_ref.dtype))
    row = lax.broadcasted_iota(jnp.int32, (LANES, LANES), 0)
    lane = lax.broadcasted_iota(jnp.int32, (LANES, LANES), 1)
    keep = lane <= row
    zero = jnp.zeros((LANES, LANES), jnp.float32)
    strip_ref[0:LANES, :] = zero.astype(strip_ref.dtype)

    def step(q, before):
        line = jnp.broadcast_to(turned_ref[pl.ds(q, 1), :], (LANES, LANES))
        here = pltpu.roll(line, 1, 1, stride=1, stride_axis=0)
        at = pl.multiple_of((q + 1) * LANES, LANES)
        strip_ref[pl.ds(at, LANES), :] = jnp.where(keep, here, before).astype(strip_ref.dtype)
        return here

    lax.fori_loop(0, count, step, zero)


def toeplitz(strip_ref, first, count):
    at = pl.multiple_of(first * BLK, BLK)
    near = strip_ref[pl.ds(at + LANES, count * BLK), :]
    far = strip_ref[pl.ds(at, count * BLK), :]
    return jnp.concatenate([near, far], axis=1)


def conv_tile(g_ref, strip_ref, acc_ref, out_ref, row, blocks, group, tile):
    rows = tile * group
    half = rows // 2
    acc_ref[...] = jnp.zeros_like(acc_ref)
    whole = blocks - row - tile // 2

    def piece(d, height):
        lhs = jnp.concatenate(
            [
                g_ref[pl.ds(pl.multiple_of(row * group + (d + u) * group, group), height), :]
                for u in range(4)
            ],
            axis=1,
        )
        acc_ref[0:height, :] += dot(lhs, toeplitz(strip_ref, d, 4))

    def main(k, carry):
        piece(k * 4, rows)
        return carry

    def tail(k, carry):
        piece(whole + k * 4, half)
        return carry

    lax.fori_loop(0, whole // 4, main, 0)
    lax.fori_loop(0, tile // 8, tail, 0)
    out_ref[pl.ds(row * group, rows), :] = acc_ref[...].astype(out_ref.dtype)


def conv_kernel(g_ref, h_ref, out_ref, padded_ref, strip_ref, turned_ref, acc_ref):
    rows = g_ref.shape[0]
    tile = 16
    blocks = h_ref.shape[0] * LANES // BLK
    group = rows // blocks
    padded_ref[0:rows, :] = g_ref[...]
    padded_ref[rows:, :] = jnp.zeros((padded_ref.shape[0] - rows, BLK), padded_ref.dtype)
    build_strip(h_ref, turned_ref, strip_ref)
    for k in range(blocks // tile):
        conv_tile(padded_ref, strip_ref, acc_ref, out_ref, k * tile, blocks, group, tile)


def conv(g, taps):
    rows = g.shape[0]
    count = taps.shape[0]
    group = rows * BLK // (count * LANES)
    return pl.pallas_call(
        conv_kernel,
        in_specs=[full(), full()],
        out_specs=full(),
        out_shape=jax.ShapeDtypeStruct((rows, BLK), jnp.bfloat16),
        scratch_shapes=[
            pltpu.VMEM((rows + 16 * group, BLK), jnp.bfloat16),
            pltpu.VMEM(((count + 1) * LANES, LANES), jnp.bfloat16),
            pltpu.VMEM((count, LANES), jnp.float32),
            pltpu.VMEM((16 * group, BLK), jnp.float32),
        ],
        compiler_params=pltpu.CompilerParams(vmem_limit_bytes=56 << 20),
        cost_estimate=pl.CostEstimate(
            flops=rows * rows // group * BLK * BLK, bytes_accessed=4 * rows * BLK, transcendentals=0
        ),
        name="conv",
    )(g, taps)


def turn_inputs(x_ref, xt_ref):
    flip = flip_matrix(BLK, x_ref.dtype)

    def step(k, carry):
        at = pl.multiple_of(k * BLK, BLK)
        turned = lax.dot_general(
            flip, x_ref[pl.ds(at, BLK), :], NT, preferred_element_type=jnp.float32
        )
        xt_ref[:, pl.ds(at, BLK)] = turned.astype(xt_ref.dtype)
        return carry

    lax.fori_loop(0, x_ref.shape[0] // BLK, step, 0)


def corr_kernel(g_ref, x_ref, lag_ref, padded_ref, xt_ref, cross_ref, part_ref):
    rows = g_ref.shape[0]
    blocks = part_ref.shape[0] // 2
    group = rows // blocks
    each = BLK // group
    padded_ref[0:rows, :] = g_ref[...]
    padded_ref[rows:, :] = jnp.zeros((padded_ref.shape[0] - rows, BLK), padded_ref.dtype)
    turn_inputs(x_ref, xt_ref)
    row = lax.broadcasted_iota(jnp.int32, (LANES, LANES), 0)
    lane = lax.broadcasted_iota(jnp.int32, (LANES, LANES), 1)
    keep = lane <= row
    zero = jnp.zeros((LANES, LANES), jnp.float32)

    def tile_sum(low, high):
        picked = jnp.where(keep, low, high)
        return jnp.sum(picked.reshape(LANES // 8, 8, LANES), axis=0)

    def turn(tile):
        return pltpu.roll(tile, 1, 1, stride=1, stride_axis=0)

    carry = (zero, zero)
    for span in range(blocks // each):
        depth = rows - span * BLK

        def step(k, carry):
            even, odd_half = carry
            d = span * each + k
            at = pl.multiple_of(d * group, group)
            c = dot(xt_ref[:, 0:depth], padded_ref[pl.ds(at, depth), :])
            odd = turn(odd_half + c[0:LANES, 0:LANES])
            here = turn(c[LANES:, 0:LANES] + c[0:LANES, LANES:])
            part_ref[jnp.maximum(2 * d - 2, 0)] = tile_sum(even, odd)
            part_ref[jnp.maximum(2 * d - 1, 0)] = tile_sum(odd, here)
            return here, c[LANES:, LANES:]

        carry = lax.fori_loop(0, each, step, carry)
    even, odd_half = carry
    odd = turn(odd_half)
    part_ref[2 * blocks - 2] = tile_sum(even, odd)
    part_ref[2 * blocks - 1] = tile_sum(odd, zero)
    lag_ref[...] = jnp.sum(part_ref[...], axis=1)


def corr(g, x, blocks):
    rows = g.shape[0]
    return pl.pallas_call(
        corr_kernel,
        in_specs=[full(), full()],
        out_specs=full(),
        out_shape=jax.ShapeDtypeStruct((2 * blocks, LANES), jnp.float32),
        scratch_shapes=[
            pltpu.VMEM((rows + BLK, BLK), jnp.bfloat16),
            pltpu.VMEM((BLK, rows), jnp.bfloat16),
            pltpu.VMEM((BLK, BLK), jnp.float32),
            pltpu.VMEM((2 * blocks, 8, LANES), jnp.float32),
        ],
        compiler_params=pltpu.CompilerParams(vmem_limit_bytes=56 << 20),
        cost_estimate=pl.CostEstimate(
            flops=rows * rows // (rows // blocks) * BLK * BLK,
            bytes_accessed=4 * rows * BLK,
            transcendentals=0,
        ),
        name="corr",
    )(g, x)


def on_device(inputs, grad_out, conv_filter):
    peers = lax.axis_size("seq")
    local = inputs.shape[1]
    blocks = local * peers // BLK
    taps = lax.all_gather(conv_filter, "seq", axis=0, tiled=True).reshape(-1, LANES)

    def spread(x):
        sent = split(x, peers)
        rows = sent.shape[1] * sent.shape[2]
        sent = sent.reshape(peers, rows, BLK)
        got = lax.all_to_all(sent, "seq", split_axis=0, concat_axis=0, tiled=True)
        return got.reshape(peers * rows, BLK)

    g = spread(grad_out[0])
    x = spread(inputs[0])
    y = conv(g, taps)
    y = y.reshape(peers, -1, BLK)
    back = lax.all_to_all(y, "seq", split_axis=0, concat_axis=0, tiled=True)
    back = back.reshape(peers, local // BLK, -1, BLK)
    lags = corr(g, x, blocks)
    lags = lax.psum_scatter(lags, "seq", scatter_dimension=0, tiled=True)
    lags = lax.psum(lags, "dp")
    return join(back)[None], lags.reshape(local)


def solution(mesh):
    placed = (P("dp", "seq", None), P("dp", "seq", None), P("seq"))
    return jax.shard_map(
        on_device,
        mesh=mesh,
        in_specs=placed,
        out_specs=(P("dp", "seq", None), P("seq")),
        check_vma=False,
    )
```

```python
import functools

import jax
import jax.numpy as jnp
from jax import lax
from jax.experimental import pallas as pl
from jax.experimental.pallas import tpu as pltpu
from jax.sharding import PartitionSpec as P

BLK = 256
LANES = 128
WIDE = 8
TILE = 16
NT = (((1,), (1,)), ((), ()))
MESH = pl.DeviceIdType.MESH


def dot(a, b):
    return jnp.dot(a, b, preferred_element_type=jnp.float32)


def flip_matrix(size, dtype):
    row = lax.broadcasted_iota(jnp.int32, (size, size), 0)
    col = lax.broadcasted_iota(jnp.int32, (size, size), 1)
    return jnp.where(row + col == size - 1, 1.0, 0.0).astype(dtype)


def spread(tile):
    return pltpu.roll(tile, 1, 1, stride=1, stride_axis=0)


def lower_mask():
    row = lax.broadcasted_iota(jnp.int32, (LANES, LANES), 0)
    lane = lax.broadcasted_iota(jnp.int32, (LANES, LANES), 1)
    return lane <= row


def build_strip(taps_ref, turned_ref, strip_ref):
    count = taps_ref.shape[0]
    turned_ref[...] = dot(taps_ref[...], flip_matrix(LANES, taps_ref.dtype))
    keep = lower_mask()
    zero = jnp.zeros((LANES, LANES), jnp.float32)
    strip_ref[0:LANES, :] = zero.astype(strip_ref.dtype)

    def step(q, before):
        here = spread(jnp.broadcast_to(turned_ref[pl.ds(q, 1), :], (LANES, LANES)))
        at = pl.multiple_of((q + 1) * LANES, LANES)
        strip_ref[pl.ds(at, LANES), :] = jnp.where(keep, here, before).astype(strip_ref.dtype)
        return here

    lax.fori_loop(0, count, step, zero)


def toeplitz(strip_ref, first, count):
    at = pl.multiple_of(first * BLK, BLK)
    near = strip_ref[pl.ds(at + LANES, count * BLK), :]
    far = strip_ref[pl.ds(at, count * BLK), :]
    return jnp.concatenate([near, far], axis=1)


def conv_tile(g_ref, strip_ref, acc_ref, y_ref, q, row, blocks, group):
    rows = TILE * group
    acc_ref[...] = jnp.zeros_like(acc_ref)
    whole = blocks - row - TILE // 2

    def piece(d, height):
        parts = []
        for u in range(WIDE):
            at = pl.multiple_of((row + d + u) * group, group)
            parts += [g_ref[q, 0, pl.ds(at, height), :], g_ref[q, 1, pl.ds(at, height), :]]
        acc_ref[0:height, :] += dot(jnp.concatenate(parts, axis=1), toeplitz(strip_ref, d, WIDE))

    def main(k, carry):
        piece(k * WIDE, rows)
        return carry

    lax.fori_loop(0, whole // WIDE, main, 0)
    piece(whole, rows // 2)
    done = acc_ref[...].astype(y_ref.dtype)
    y_ref[q, 0, row * group : row * group + rows, :] = done[:, 0:LANES]
    y_ref[q, 1, row * group : row * group + rows, :] = done[:, LANES:]


def turn_inputs(x_ref, xt_ref, q):
    flip = flip_matrix(BLK, x_ref.dtype)

    def step(k, carry):
        at = pl.multiple_of(k * BLK, BLK)
        block = jnp.concatenate(
            [x_ref[q, 0, pl.ds(at, BLK), :], x_ref[q, 1, pl.ds(at, BLK), :]], axis=1
        )
        turned = lax.dot_general(flip, block, NT, preferred_element_type=jnp.float32)
        turned = turned.astype(xt_ref.dtype)
        xt_ref[2 * k] = turned[:, 0:LANES]
        xt_ref[2 * k + 1] = turned[:, LANES:]
        return carry

    lax.fori_loop(0, x_ref.shape[2] // BLK, step, 0)


def cross(g_ref, xt_ref, q, d, depth, group):
    at = pl.multiple_of(d * group, group)
    left = jnp.concatenate([xt_ref[k] for k in range(depth // LANES)], axis=1)
    right = jnp.concatenate(
        [g_ref[q, 0, pl.ds(at, depth), :], g_ref[q, 1, pl.ds(at, depth), :]], axis=1
    )
    return dot(left, right)


def corr_first(g_ref, xt_ref, cross_ref, blocks, group):
    each = BLK // group
    for span in range(blocks // each):
        depth = blocks * group - span * BLK

        def step(k, carry):
            for u in range(2):
                d = span * each + 2 * k + u
                cross_ref[d] = cross(g_ref, xt_ref, 0, d, depth, group)
            return carry

        lax.fori_loop(0, each // 2, step, 0)


def corr_last(g_ref, xt_ref, cross_ref, part_ref, lag_ref, blocks, group):
    each = BLK // group
    keep = lower_mask()
    zero = jnp.zeros((LANES, LANES), jnp.float32)

    def tile_sum(low, high):
        picked = jnp.where(keep, low, high)
        return jnp.sum(picked.reshape(LANES // 8, 8, LANES), axis=0)

    carry = (zero, zero)
    for span in range(blocks // each):
        depth = blocks * group - span * BLK

        def step(k, carry):
            even, half = carry
            for u in range(2):
                d = span * each + 2 * k + u
                c = cross_ref[d] + cross(g_ref, xt_ref, 1, d, depth, group)
                odd = spread(half + c[0:LANES, 0:LANES])
                here = spread(c[LANES:, 0:LANES] + c[0:LANES, LANES:])
                part_ref[jnp.maximum(2 * d - 2, 0)] = tile_sum(even, odd)
                part_ref[jnp.maximum(2 * d - 1, 0)] = tile_sum(odd, here)
                even, half = here, c[LANES:, LANES:]
            return even, half

        carry = lax.fori_loop(0, each // 2, step, carry)
    even, half = carry
    odd = spread(half)
    part_ref[2 * blocks - 2] = tile_sum(even, odd)
    part_ref[2 * blocks - 1] = tile_sum(odd, zero)
    lag_ref[...] = jnp.sum(part_ref[...], axis=1)


def kernel(
    peers,
    rings,
    x_hbm,
    g_hbm,
    h_ref,
    y_hbm,
    lag_out,
    gin,
    xin,
    sent_g,
    sent_x,
    taps,
    turned,
    strip,
    got_g,
    got_x,
    xt,
    acc,
    cross_sums,
    part,
    lag,
    y_rows,
    got_y,
    yout,
    got_lag,
    lag_mine,
    got_ring,
    send_sems,
    recv_sems,
    local_sems,
):
    me = lax.axis_index("seq")
    ring = lax.axis_index("dp")
    local, channels = gin.shape
    near = local // BLK
    blocks = near * peers
    group = channels // 2 // peers
    held = near * group

    def other(k):
        return lax.rem(me + k, peers)

    load_g = pltpu.make_async_copy(g_hbm, gin, local_sems.at[0])
    load_x = pltpu.make_async_copy(x_hbm, xin, local_sems.at[1])
    load_g.start()
    load_x.start()

    barrier = pltpu.get_barrier_semaphore()

    def greet(k, carry):
        pl.semaphore_signal(barrier, inc=1, device_id=(ring, other(k)), device_id_type=MESH)
        return carry

    def greet_ring(k, carry):
        to = lax.rem(ring + k, rings)
        pl.semaphore_signal(barrier, inc=1, device_id=(to, me), device_id_type=MESH)
        return carry

    lax.fori_loop(1, peers, greet, 0)
    lax.fori_loop(1, rings, greet_ring, 0)

    def turn(in_ref, sent_ref, q):
        for k in range(near):
            block = jnp.transpose(in_ref[k * BLK : (k + 1) * BLK, q * BLK : (q + 1) * BLK])
            for p in range(peers):
                for side in range(2):
                    sent_ref[q, p, side, k * group : (k + 1) * group, :] = block[
                        p * group : (p + 1) * group, side * LANES : (side + 1) * LANES
                    ]

    def mine(rows):
        return pl.ds(pl.multiple_of(me * rows, rows), rows)

    def send(stage, source, target, to):
        pltpu.make_async_remote_copy(
            src_ref=source,
            dst_ref=target,
            send_sem=send_sems.at[stage],
            recv_sem=recv_sems.at[stage],
            device_id=(ring, to),
            device_id_type=MESH,
        ).start()

    def drain(stage, sent, got):
        if sent is not None:
            pltpu.make_async_copy(sent, sent, send_sems.at[stage]).wait()
        if got is not None:
            pltpu.make_async_copy(got, got, recv_sems.at[stage]).wait()

    def send_half(stage, sent_ref, got_ref, q):
        def step(k, carry):
            to = other(k)
            send(stage, sent_ref.at[q, to], got_ref.at[q, :, mine(held), :], to)
            return carry

        lax.fori_loop(1, peers, step, 0)
        got_ref[q, :, mine(held), :] = sent_ref[q, me]

    others = (peers - 1) * held

    load_g.wait()
    turn(gin, sent_g, 0)
    pl.semaphore_wait(barrier, peers + rings - 2)

    eight = h_ref.shape[0]

    def send_taps(k, carry):
        to = other(k)
        send(0, h_ref, taps.at[mine(eight), :], to)
        return carry

    lax.fori_loop(1, peers, send_taps, 0)
    send_half(1, sent_g, got_g, 0)
    taps[mine(eight), :] = h_ref[...]
    turn(gin, sent_g, 1)
    load_x.wait()
    turn(xin, sent_x, 0)
    send_half(2, sent_g, got_g, 1)
    turn(xin, sent_x, 1)
    send_half(3, sent_x, got_x, 0)

    pad = got_g.shape[2] - blocks * group
    got_g[:, :, blocks * group :, :] = jnp.zeros((2, 2, pad, LANES), got_g.dtype)
    send_half(4, sent_x, got_x, 1)

    drain(0, None, taps.at[0 : (peers - 1) * eight, :])
    build_strip(taps, turned, strip)

    for q in range(2):
        drain(1 + q, None, got_g.at[q, :, 0:others, :])
        for row in range(0, blocks, TILE):
            conv_tile(got_g, strip, acc, y_rows, q, row, blocks, group)

            def send_rows(p, carry):
                @pl.when(p != me)
                def _():
                    at = pl.multiple_of(p * held, held)
                    send(5 + q, y_rows.at[q, :, pl.ds(at, held), :], got_y.at[q, me], p)

                return carry

            lax.fori_loop(row // near, (row + TILE) // near, send_rows, 0)
        got_y[q, me] = y_rows[q, :, mine(held), :]

    drain(3, None, got_x.at[0, :, 0:others, :])
    turn_inputs(got_x, xt, 0)
    corr_first(got_g, xt, cross_sums, blocks, group)
    drain(4, None, got_x.at[1, :, 0:others, :])
    turn_inputs(got_x, xt, 1)
    corr_last(got_g, xt, cross_sums, part, lag, blocks, group)

    def send_lags(k, carry):
        to = other(k)
        source = lag.at[pl.ds(pl.multiple_of(to * eight, eight), eight), :]
        send(7, source, got_lag.at[me], to)
        return carry

    lax.fori_loop(1, peers, send_lags, 0)
    got_lag[me] = lag[mine(eight), :]

    for q in range(2):
        drain(5 + q, None, got_y.at[q, 0 : peers - 1])
        for k in range(near):
            for side in range(2):
                rows = got_y[q, :, side, k * group : (k + 1) * group, :].reshape(BLK, LANES)
                at = k * BLK + side * LANES
                yout[at : at + LANES, q * BLK : (q + 1) * BLK] = jnp.transpose(rows)

    drain(7, None, got_lag.at[0 : peers - 1])
    lag_mine[...] = jnp.sum(got_lag[...], axis=0)

    def send_ring(k, carry):
        to = lax.rem(ring + k, rings)
        pltpu.make_async_remote_copy(
            src_ref=lag_mine,
            dst_ref=got_ring.at[ring],
            send_sem=send_sems.at[8],
            recv_sem=recv_sems.at[8],
            device_id=(to, me),
            device_id_type=MESH,
        ).start()
        return carry

    lax.fori_loop(1, rings, send_ring, 0)
    store_y = pltpu.make_async_copy(yout, y_hbm, local_sems.at[2])
    store_y.start()
    got_ring[ring] = lag_mine[...]

    drain(0, taps.at[0 : (peers - 1) * eight, :], None)
    for q in range(2):
        drain(1 + q, sent_g.at[q, 0 : peers - 1], None)
        drain(3 + q, sent_x.at[q, 0 : peers - 1], None)
        drain(5 + q, y_rows.at[q, :, 0:others, :], None)
    drain(7, lag.at[0 : (peers - 1) * eight, :], None)
    if rings > 1:
        drain(8, got_ring.at[0 : rings - 1], got_ring.at[0 : rings - 1])
    lag_out[...] = jnp.sum(got_ring[...], axis=0)
    store_y.wait()


def on_device(inputs, grad_out, conv_filter):
    peers = lax.axis_size("seq")
    rings = lax.axis_size("dp")
    local, channels = inputs.shape[1:]
    taps = local * peers
    blocks = taps // BLK
    group = channels // 2 // peers
    near = local // BLK
    rows = blocks * group
    held = near * group
    eight = local // LANES
    half = jnp.bfloat16
    whole = jnp.float32
    anywhere = pl.BlockSpec(memory_space=pl.ANY)
    inside = pl.BlockSpec(memory_space=pltpu.VMEM)
    y, lags = pl.pallas_call(
        functools.partial(kernel, peers, rings),
        in_specs=[anywhere, anywhere, inside],
        out_specs=[anywhere, inside],
        out_shape=[
            jax.ShapeDtypeStruct((local, channels), half),
            jax.ShapeDtypeStruct((eight, LANES), whole),
        ],
        scratch_shapes=[
            pltpu.VMEM((local, channels), half),
            pltpu.VMEM((local, channels), half),
            pltpu.VMEM((2, peers, 2, held, LANES), half),
            pltpu.VMEM((2, peers, 2, held, LANES), half),
            pltpu.VMEM((taps // LANES, LANES), half),
            pltpu.VMEM((taps // LANES, LANES), whole),
            pltpu.VMEM((taps + LANES, LANES), half),
            pltpu.VMEM((2, 2, rows + BLK, LANES), half),
            pltpu.VMEM((2, 2, rows, LANES), half),
            pltpu.VMEM((rows // LANES, BLK, LANES), half),
            pltpu.VMEM((TILE * group, BLK), whole),
            pltpu.VMEM((blocks, BLK, BLK), whole),
            pltpu.VMEM((2 * blocks, 8, LANES), whole),
            pltpu.VMEM((2 * blocks, LANES), whole),
            pltpu.VMEM((2, 2, rows, LANES), half),
            pltpu.VMEM((2, peers, 2, held, LANES), half),
            pltpu.VMEM((local, channels), half),
            pltpu.VMEM((peers, eight, LANES), whole),
            pltpu.VMEM((eight, LANES), whole),
            pltpu.VMEM((rings, eight, LANES), whole),
            pltpu.SemaphoreType.DMA((9,)),
            pltpu.SemaphoreType.DMA((9,)),
            pltpu.SemaphoreType.DMA((3,)),
        ],
        compiler_params=pltpu.CompilerParams(
            collective_id=0, has_side_effects=True, vmem_limit_bytes=56 << 20
        ),
        name="hyena_backward",
    )(inputs[0], grad_out[0], conv_filter.reshape(eight, LANES))
    return y[None], lags.reshape(local)


def solution(mesh):
    placed = (P("dp", "seq", None), P("dp", "seq", None), P("seq"))
    return jax.shard_map(
        on_device,
        mesh=mesh,
        in_specs=placed,
        out_specs=(P("dp", "seq", None), P("seq")),
        check_vma=False,
    )
```

```python
import functools

import jax
import jax.numpy as jnp
from jax import lax
from jax.experimental import pallas as pl
from jax.experimental.pallas import tpu as pltpu
from jax.sharding import PartitionSpec as P

BLK = 256
LANES = 128
DEEP = 8
TILE = 16
NT = (((1,), (1,)), ((), ()))
MESH = pl.DeviceIdType.MESH


def dot(a, b):
    return jnp.dot(a, b, preferred_element_type=jnp.float32)


def flip_matrix(size, dtype):
    row = lax.broadcasted_iota(jnp.int32, (size, size), 0)
    col = lax.broadcasted_iota(jnp.int32, (size, size), 1)
    return jnp.where(row + col == size - 1, 1.0, 0.0).astype(dtype)


def spread(tile):
    return pltpu.roll(tile, 1, 1, stride=1, stride_axis=0)


def lower_mask():
    row = lax.broadcasted_iota(jnp.int32, (LANES, LANES), 0)
    lane = lax.broadcasted_iota(jnp.int32, (LANES, LANES), 1)
    return lane <= row


def build_strip(taps_ref, turned_ref, strip_ref):
    count = taps_ref.shape[0]
    unroll = 8
    turned_ref[...] = dot(taps_ref[...], flip_matrix(LANES, taps_ref.dtype))
    keep = lower_mask()
    zero = jnp.zeros((LANES, LANES), jnp.float32)
    strip_ref[0:LANES, :] = zero.astype(strip_ref.dtype)

    def step(k, before):
        for u in range(unroll):
            q = k * unroll + u
            here = spread(jnp.broadcast_to(turned_ref[pl.ds(q, 1), :], (LANES, LANES)))
            at = pl.multiple_of((q + 1) * LANES, LANES)
            strip_ref[pl.ds(at, LANES), :] = jnp.where(keep, here, before).astype(strip_ref.dtype)
            before = here
        return before

    lax.fori_loop(0, count // unroll, step, zero)


def toeplitz(strip_ref, first, count):
    at = pl.multiple_of(first * BLK, BLK)
    near = strip_ref[pl.ds(at + LANES, count * BLK), :]
    far = strip_ref[pl.ds(at, count * BLK), :]
    return jnp.concatenate([near, far], axis=1)


def conv_tile(g_ref, strip_ref, acc_ref, y_ref, q, row, blocks, group):
    rows = TILE * group
    acc_ref[...] = jnp.zeros_like(acc_ref)
    half = TILE // 2

    def piece(d, count, height):
        parts = []
        for u in range(count):
            at = pl.multiple_of((row + d + u) * group, group)
            parts += [g_ref[q, 0, pl.ds(at, height), :], g_ref[q, 1, pl.ds(at, height), :]]
        return dot(jnp.concatenate(parts, axis=1), toeplitz(strip_ref, d, count))

    def main(k, carry):
        acc_ref[...] += piece(k * TILE, TILE, rows)
        return carry

    left = blocks - row - TILE
    lax.fori_loop(0, left // TILE, main, 0)
    acc_ref[...] += piece(left, half, rows)
    acc_ref[0 : rows // 2, :] += piece(left + half, half, rows // 2)
    done = acc_ref[...].astype(y_ref.dtype)
    y_ref[q, 0, row * group : row * group + rows, :] = done[:, 0:LANES]
    y_ref[q, 1, row * group : row * group + rows, :] = done[:, LANES:]


def turn_inputs(x_ref, xt_ref, q):
    flip = flip_matrix(BLK, x_ref.dtype)

    def step(k, carry):
        at = pl.multiple_of(k * BLK, BLK)
        block = jnp.concatenate(
            [x_ref[q, 0, pl.ds(at, BLK), :], x_ref[q, 1, pl.ds(at, BLK), :]], axis=1
        )
        turned = lax.dot_general(flip, block, NT, preferred_element_type=jnp.float32)
        turned = turned.astype(xt_ref.dtype)
        xt_ref[2 * k] = turned[:, 0:LANES]
        xt_ref[2 * k + 1] = turned[:, LANES:]
        return carry

    lax.fori_loop(0, x_ref.shape[2] // BLK, step, 0)


def cross(g_ref, xt_ref, q, d, depth, group):
    at = pl.multiple_of(d * group, group)
    left = jnp.concatenate([xt_ref[k] for k in range(depth // LANES)], axis=1)
    right = jnp.concatenate(
        [g_ref[q, 0, pl.ds(at, depth), :], g_ref[q, 1, pl.ds(at, depth), :]], axis=1
    )
    return dot(left, right)


def corr_first(g_ref, xt_ref, cross_ref, blocks, group, after):
    each = BLK // group
    for span in range(blocks // each):
        depth = blocks * group - span * BLK

        def step(k, carry):
            for u in range(DEEP):
                d = span * each + DEEP * k + u
                cross_ref[d] = cross(g_ref, xt_ref, 0, d, depth, group)
            return carry

        lax.fori_loop(0, each // DEEP, step, 0)
        after(span)


def corr_last(g_ref, xt_ref, cross_ref, part_ref, lag_ref, blocks, group):
    each = BLK // group
    keep = lower_mask()
    zero = jnp.zeros((LANES, LANES), jnp.float32)

    def tile_sum(low, high):
        picked = jnp.where(keep, low, high)
        return jnp.sum(picked.reshape(LANES // 8, 8, LANES), axis=0)

    carry = (zero, zero)
    for span in range(blocks // each):
        depth = blocks * group - span * BLK

        def step(k, carry):
            even, half = carry
            for u in range(DEEP):
                d = span * each + DEEP * k + u
                c = cross_ref[d] + cross(g_ref, xt_ref, 1, d, depth, group)
                odd = spread(half + c[0:LANES, 0:LANES])
                here = spread(c[LANES:, 0:LANES] + c[0:LANES, LANES:])
                part_ref[jnp.maximum(2 * d - 2, 0)] = tile_sum(even, odd)
                part_ref[jnp.maximum(2 * d - 1, 0)] = tile_sum(odd, here)
                even, half = here, c[LANES:, LANES:]
            return even, half

        carry = lax.fori_loop(0, each // DEEP, step, carry)
    even, half = carry
    odd = spread(half)
    part_ref[2 * blocks - 2] = tile_sum(even, odd)
    part_ref[2 * blocks - 1] = tile_sum(odd, zero)
    lag_ref[...] = jnp.sum(part_ref[...], axis=1)


def kernel(
    peers,
    rings,
    x_hbm,
    g_hbm,
    h_ref,
    y_hbm,
    lag_out,
    gin,
    xin,
    sent_g,
    sent_x,
    taps,
    turned,
    strip,
    got_g,
    got_x,
    xt,
    acc,
    cross_sums,
    part,
    lag,
    y_rows,
    got_y,
    yout,
    got_lag,
    lag_mine,
    got_ring,
    send_sems,
    recv_sems,
    local_sems,
):
    me = lax.axis_index("seq")
    ring = lax.axis_index("dp")
    local, channels = gin.shape
    near = local // BLK
    blocks = near * peers
    group = channels // 2 // peers
    held = near * group

    def other(k):
        return lax.rem(me + k, peers)

    def load(k, source, target, cols):
        copy = pltpu.make_async_copy(source.at[:, cols], target.at[:, cols], local_sems.at[k])
        copy.start()
        return copy

    early, late = pl.ds(0, BLK), pl.ds(BLK, BLK)
    loads = [
        load(0, g_hbm, gin, early),
        load(1, g_hbm, gin, late),
        load(2, x_hbm, xin, early),
        load(3, x_hbm, xin, late),
    ]

    barrier = pltpu.get_barrier_semaphore()

    def greet(k, carry):
        pl.semaphore_signal(barrier, inc=1, device_id=(ring, other(k)), device_id_type=MESH)
        return carry

    def greet_ring(k, carry):
        to = lax.rem(ring + k, rings)
        pl.semaphore_signal(barrier, inc=1, device_id=(to, me), device_id_type=MESH)
        return carry

    lax.fori_loop(1, peers, greet, 0)
    lax.fori_loop(1, rings, greet_ring, 0)

    def turn(in_ref, sent_ref, q):
        for k in range(near):
            block = jnp.transpose(in_ref[k * BLK : (k + 1) * BLK, q * BLK : (q + 1) * BLK])
            for p in range(peers):
                for side in range(2):
                    sent_ref[q, p, side, k * group : (k + 1) * group, :] = block[
                        p * group : (p + 1) * group, side * LANES : (side + 1) * LANES
                    ]

    def mine(rows):
        return pl.ds(pl.multiple_of(me * rows, rows), rows)

    def send(stage, source, target, to):
        pltpu.make_async_remote_copy(
            src_ref=source,
            dst_ref=target,
            send_sem=send_sems.at[stage],
            recv_sem=recv_sems.at[stage],
            device_id=(ring, to),
            device_id_type=MESH,
        ).start()

    def drain(stage, sent, got):
        if sent is not None:
            pltpu.make_async_copy(sent, sent, send_sems.at[stage]).wait()
        if got is not None:
            pltpu.make_async_copy(got, got, recv_sems.at[stage]).wait()

    def send_half(stage, sent_ref, got_ref, q):
        def step(k, carry):
            to = other(k)
            send(stage, sent_ref.at[q, to], got_ref.at[q, :, mine(held), :], to)
            return carry

        lax.fori_loop(1, peers, step, 0)
        got_ref[q, :, mine(held), :] = sent_ref[q, me]

    others = (peers - 1) * held

    loads[0].wait()
    turn(gin, sent_g, 0)
    pl.semaphore_wait(barrier, peers + rings - 2)

    eight = h_ref.shape[0]

    def send_taps(k, carry):
        to = other(k)
        send(0, h_ref, taps.at[mine(eight), :], to)
        return carry

    lax.fori_loop(1, peers, send_taps, 0)
    send_half(1, sent_g, got_g, 0)
    taps[mine(eight), :] = h_ref[...]
    loads[1].wait()
    turn(gin, sent_g, 1)
    loads[2].wait()
    turn(xin, sent_x, 0)
    loads[3].wait()
    turn(xin, sent_x, 1)
    pad = got_g.shape[2] - blocks * group
    got_g[:, :, blocks * group :, :] = jnp.zeros((2, 2, pad, LANES), got_g.dtype)

    def send_rows(q):
        def step(k, carry):
            to = other(k)
            at = pl.multiple_of(to * held, held)
            send(5 + q, y_rows.at[q, :, pl.ds(at, held), :], got_y.at[q, me], to)
            return carry

        lax.fori_loop(1, peers, step, 0)
        got_y[q, me] = y_rows[q, :, mine(held), :]

    def finish_rows(q):
        drain(5 + q, None, got_y.at[q, 0 : peers - 1])
        for k in range(near):
            for side in range(2):
                rows = got_y[q, :, side, k * group : (k + 1) * group, :].reshape(BLK, LANES)
                at = k * BLK + side * LANES
                yout[at : at + LANES, q * BLK : (q + 1) * BLK] = jnp.transpose(rows)
        cols = early if q == 0 else late
        copy = pltpu.make_async_copy(yout.at[:, cols], y_hbm.at[:, cols], local_sems.at[4 + q])
        copy.start()
        return copy

    drain(0, None, taps.at[0 : (peers - 1) * eight, :])
    build_strip(taps, turned, strip)
    send_half(2, sent_g, got_g, 1)

    tiles = range(0, blocks, TILE)
    drain(1, None, got_g.at[0, :, 0:others, :])
    for row in tiles:
        conv_tile(got_g, strip, acc, y_rows, 0, row, blocks, group)
        if row == 0:
            send_half(3, sent_x, got_x, 0)

    drain(2, None, got_g.at[1, :, 0:others, :])
    for row in tiles:
        conv_tile(got_g, strip, acc, y_rows, 1, row, blocks, group)
        if row == 0:
            send_half(4, sent_x, got_x, 1)
    send_rows(0)

    def after(span):
        if span == min(1, blocks * group // BLK - 1):
            send_rows(1)

    drain(3, None, got_x.at[0, :, 0:others, :])
    turn_inputs(got_x, xt, 0)
    corr_first(got_g, xt, cross_sums, blocks, group, after)
    drain(4, None, got_x.at[1, :, 0:others, :])
    turn_inputs(got_x, xt, 1)
    corr_last(got_g, xt, cross_sums, part, lag, blocks, group)

    def send_lags(k, carry):
        to = other(k)
        source = lag.at[pl.ds(pl.multiple_of(to * eight, eight), eight), :]
        send(7, source, got_lag.at[me], to)
        return carry

    lax.fori_loop(1, peers, send_lags, 0)
    got_lag[me] = lag[mine(eight), :]

    stores = [finish_rows(0), finish_rows(1)]
    drain(7, None, got_lag.at[0 : peers - 1])
    lag_mine[...] = jnp.sum(got_lag[...], axis=0)

    def send_ring(k, carry):
        to = lax.rem(ring + k, rings)
        pltpu.make_async_remote_copy(
            src_ref=lag_mine,
            dst_ref=got_ring.at[ring],
            send_sem=send_sems.at[8],
            recv_sem=recv_sems.at[8],
            device_id=(to, me),
            device_id_type=MESH,
        ).start()
        return carry

    lax.fori_loop(1, rings, send_ring, 0)
    got_ring[ring] = lag_mine[...]

    drain(0, taps.at[0 : (peers - 1) * eight, :], None)
    for q in range(2):
        drain(1 + q, sent_g.at[q, 0 : peers - 1], None)
        drain(3 + q, sent_x.at[q, 0 : peers - 1], None)
        drain(5 + q, y_rows.at[q, :, 0:others, :], None)
    drain(7, lag.at[0 : (peers - 1) * eight, :], None)
    if rings > 1:
        drain(8, got_ring.at[0 : rings - 1], got_ring.at[0 : rings - 1])
    lag_out[...] = jnp.sum(got_ring[...], axis=0)
    for store in stores:
        store.wait()


def on_device(inputs, grad_out, conv_filter):
    peers = lax.axis_size("seq")
    rings = lax.axis_size("dp")
    local, channels = inputs.shape[1:]
    taps = local * peers
    blocks = taps // BLK
    group = channels // 2 // peers
    near = local // BLK
    rows = blocks * group
    held = near * group
    eight = local // LANES
    half = jnp.bfloat16
    whole = jnp.float32
    anywhere = pl.BlockSpec(memory_space=pl.ANY)
    inside = pl.BlockSpec(memory_space=pltpu.VMEM)
    y, lags = pl.pallas_call(
        functools.partial(kernel, peers, rings),
        in_specs=[anywhere, anywhere, inside],
        out_specs=[anywhere, inside],
        out_shape=[
            jax.ShapeDtypeStruct((local, channels), half),
            jax.ShapeDtypeStruct((eight, LANES), whole),
        ],
        scratch_shapes=[
            pltpu.VMEM((local, channels), half),
            pltpu.VMEM((local, channels), half),
            pltpu.VMEM((2, peers, 2, held, LANES), half),
            pltpu.VMEM((2, peers, 2, held, LANES), half),
            pltpu.VMEM((taps // LANES, LANES), half),
            pltpu.VMEM((taps // LANES, LANES), whole),
            pltpu.VMEM((taps + LANES, LANES), half),
            pltpu.VMEM((2, 2, rows + BLK, LANES), half),
            pltpu.VMEM((2, 2, rows, LANES), half),
            pltpu.VMEM((rows // LANES, BLK, LANES), half),
            pltpu.VMEM((TILE * group, BLK), whole),
            pltpu.VMEM((blocks, BLK, BLK), whole),
            pltpu.VMEM((2 * blocks, 8, LANES), whole),
            pltpu.VMEM((2 * blocks, LANES), whole),
            pltpu.VMEM((2, 2, rows, LANES), half),
            pltpu.VMEM((2, peers, 2, held, LANES), half),
            pltpu.VMEM((local, channels), half),
            pltpu.VMEM((peers, eight, LANES), whole),
            pltpu.VMEM((eight, LANES), whole),
            pltpu.VMEM((rings, eight, LANES), whole),
            pltpu.SemaphoreType.DMA((9,)),
            pltpu.SemaphoreType.DMA((9,)),
            pltpu.SemaphoreType.DMA((6,)),
        ],
        compiler_params=pltpu.CompilerParams(
            collective_id=0, has_side_effects=True, vmem_limit_bytes=56 << 20
        ),
        name="hyena_backward",
    )(inputs[0], grad_out[0], conv_filter.reshape(eight, LANES))
    return y[None], lags.reshape(local)


def solution(mesh):
    placed = (P("dp", "seq", None), P("dp", "seq", None), P("seq"))
    return jax.shard_map(
        on_device,
        mesh=mesh,
        in_specs=placed,
        out_specs=(P("dp", "seq", None), P("seq")),
        check_vma=False,
    )
```

```python
import functools

import jax
import jax.numpy as jnp
from jax import lax
from jax.experimental import pallas as pl
from jax.experimental.pallas import tpu as pltpu
from jax.sharding import PartitionSpec as P

BLK = 256
LANES = 128
DEEP = 16
TILE = 16
NT = (((1,), (1,)), ((), ()))
MESH = pl.DeviceIdType.MESH


def dot(a, b):
    return jnp.dot(a, b, preferred_element_type=jnp.float32)


def flip_matrix(size, dtype):
    row = lax.broadcasted_iota(jnp.int32, (size, size), 0)
    col = lax.broadcasted_iota(jnp.int32, (size, size), 1)
    return jnp.where(row + col == size - 1, 1.0, 0.0).astype(dtype)


def spread(tile):
    return pltpu.roll(tile, 1, 1, stride=1, stride_axis=0)


def lower_mask():
    row = lax.broadcasted_iota(jnp.int32, (LANES, LANES), 0)
    lane = lax.broadcasted_iota(jnp.int32, (LANES, LANES), 1)
    return lane <= row


def build_strip(taps_ref, turned_ref, strip_ref):
    count = taps_ref.shape[0]
    unroll = 8
    turned_ref[...] = dot(taps_ref[...], flip_matrix(LANES, taps_ref.dtype))
    keep = lower_mask()
    zero = jnp.zeros((LANES, LANES), jnp.float32)
    strip_ref[0:LANES, :] = zero.astype(strip_ref.dtype)

    def step(k, before):
        for u in range(unroll):
            q = k * unroll + u
            here = spread(jnp.broadcast_to(turned_ref[pl.ds(q, 1), :], (LANES, LANES)))
            at = pl.multiple_of((q + 1) * LANES, LANES)
            strip_ref[pl.ds(at, LANES), :] = jnp.where(keep, here, before).astype(strip_ref.dtype)
            before = here
        return before

    lax.fori_loop(0, count // unroll, step, zero)


def toeplitz(strip_ref, first, count):
    at = pl.multiple_of(first * BLK, BLK)
    near = strip_ref[pl.ds(at + LANES, count * BLK), :]
    far = strip_ref[pl.ds(at, count * BLK), :]
    return jnp.concatenate([near, far], axis=1)


def conv_half(g_ref, strip_ref, acc_ref, y_ref, q, blocks, group, after):
    rows = TILE * group
    half = TILE // 2
    count = blocks // TILE

    def tile(t, carry):
        row = t * TILE
        left = blocks - row - TILE
        acc_ref[...] = jnp.zeros_like(acc_ref)

        def piece(d, width, height):
            parts = []
            for u in range(width):
                at = pl.multiple_of((row + d + u) * group, group)
                parts += [g_ref[q, 0, pl.ds(at, height), :], g_ref[q, 1, pl.ds(at, height), :]]
            return dot(jnp.concatenate(parts, axis=1), toeplitz(strip_ref, d, width))

        def main(k, carry):
            acc_ref[...] += piece(k * TILE, TILE, rows)
            return carry

        lax.fori_loop(0, count - 1 - t, main, 0)
        acc_ref[...] += piece(left, half, rows)
        acc_ref[0 : rows // 2, :] += piece(left + half, half, rows // 2)
        done = acc_ref[...].astype(y_ref.dtype)
        at = pl.multiple_of(t * rows, rows)
        y_ref[q, 0, pl.ds(at, rows), :] = done[:, 0:LANES]
        y_ref[q, 1, pl.ds(at, rows), :] = done[:, LANES:]
        pl.when(t == 0)(after)
        return carry

    lax.fori_loop(0, count, tile, 0)


def turn_inputs(x_ref, xt_ref, q):
    flip = flip_matrix(BLK, x_ref.dtype)

    def step(k, carry):
        at = pl.multiple_of(k * BLK, BLK)
        block = jnp.concatenate(
            [x_ref[q, 0, pl.ds(at, BLK), :], x_ref[q, 1, pl.ds(at, BLK), :]], axis=1
        )
        turned = lax.dot_general(flip, block, NT, preferred_element_type=jnp.float32)
        turned = turned.astype(xt_ref.dtype)
        xt_ref[2 * k] = turned[:, 0:LANES]
        xt_ref[2 * k + 1] = turned[:, LANES:]
        return carry

    lax.fori_loop(0, x_ref.shape[2] // BLK, step, 0)


def cross(g_ref, xt_ref, q, d, depth, group):
    at = pl.multiple_of(d * group, group)
    left = jnp.concatenate([xt_ref[k] for k in range(depth // LANES)], axis=1)
    right = jnp.concatenate(
        [g_ref[q, 0, pl.ds(at, depth), :], g_ref[q, 1, pl.ds(at, depth), :]], axis=1
    )
    return dot(left, right)


def corr_first(g_ref, xt_ref, cross_ref, blocks, group, after):
    each = BLK // group
    for span in range(blocks // each):
        depth = blocks * group - span * BLK

        def step(k, carry):
            for u in range(DEEP):
                d = span * each + DEEP * k + u
                cross_ref[d] = cross(g_ref, xt_ref, 0, d, depth, group)
            return carry

        lax.fori_loop(0, each // DEEP, step, 0)
        after(span)


def corr_last(g_ref, xt_ref, cross_ref, part_ref, lag_ref, blocks, group):
    each = BLK // group
    keep = lower_mask()
    zero = jnp.zeros((LANES, LANES), jnp.float32)

    def tile_sum(low, high):
        picked = jnp.where(keep, low, high)
        return jnp.sum(picked.reshape(LANES // 8, 8, LANES), axis=0)

    carry = (zero, zero)
    for span in range(blocks // each):
        depth = blocks * group - span * BLK

        def step(k, carry):
            even, half = carry
            for u in range(DEEP):
                d = span * each + DEEP * k + u
                c = cross_ref[d] + cross(g_ref, xt_ref, 1, d, depth, group)
                odd = spread(half + c[0:LANES, 0:LANES])
                here = spread(c[LANES:, 0:LANES] + c[0:LANES, LANES:])
                part_ref[jnp.maximum(2 * d - 2, 0)] = tile_sum(even, odd)
                part_ref[jnp.maximum(2 * d - 1, 0)] = tile_sum(odd, here)
                even, half = here, c[LANES:, LANES:]
            return even, half

        carry = lax.fori_loop(0, each // DEEP, step, carry)
    even, half = carry
    odd = spread(half)
    part_ref[2 * blocks - 2] = tile_sum(even, odd)
    part_ref[2 * blocks - 1] = tile_sum(odd, zero)
    lag_ref[...] = jnp.sum(part_ref[...], axis=1)


def kernel(
    peers,
    rings,
    x_hbm,
    g_hbm,
    h_ref,
    y_hbm,
    lag_out,
    gin,
    xin,
    sent_g,
    sent_x,
    taps,
    turned,
    strip,
    got_g,
    got_x,
    xt,
    acc,
    cross_sums,
    part,
    lag,
    y_rows,
    got_y,
    yout,
    got_lag,
    lag_mine,
    got_ring,
    send_sems,
    recv_sems,
    local_sems,
):
    me = lax.axis_index("seq")
    ring = lax.axis_index("dp")
    local, channels = gin.shape
    near = local // BLK
    blocks = near * peers
    group = channels // 2 // peers
    held = near * group

    def other(k):
        return lax.rem(me + k, peers)

    def load(k, source, target, cols):
        copy = pltpu.make_async_copy(source.at[:, cols], target.at[:, cols], local_sems.at[k])
        copy.start()
        return copy

    early, late = pl.ds(0, BLK), pl.ds(BLK, BLK)
    loads = [
        load(0, g_hbm, gin, early),
        load(1, g_hbm, gin, late),
        load(2, x_hbm, xin, early),
        load(3, x_hbm, xin, late),
    ]

    barrier = pltpu.get_barrier_semaphore()

    def greet(k, carry):
        pl.semaphore_signal(barrier, inc=1, device_id=(ring, other(k)), device_id_type=MESH)
        return carry

    def greet_ring(k, carry):
        to = lax.rem(ring + k, rings)
        pl.semaphore_signal(barrier, inc=1, device_id=(to, me), device_id_type=MESH)
        return carry

    lax.fori_loop(1, peers, greet, 0)
    lax.fori_loop(1, rings, greet_ring, 0)

    def turn(in_ref, sent_ref, q):
        def step(k, carry):
            at = pl.multiple_of(k * BLK, BLK)
            to = pl.multiple_of(k * group, group)
            block = jnp.transpose(in_ref[pl.ds(at, BLK), q * BLK : (q + 1) * BLK])
            for p in range(peers):
                for side in range(2):
                    sent_ref[q, p, side, pl.ds(to, group), :] = block[
                        p * group : (p + 1) * group, side * LANES : (side + 1) * LANES
                    ]
            return carry

        lax.fori_loop(0, near, step, 0)

    def mine(rows):
        return pl.ds(pl.multiple_of(me * rows, rows), rows)

    def send(stage, source, target, to):
        pltpu.make_async_remote_copy(
            src_ref=source,
            dst_ref=target,
            send_sem=send_sems.at[stage],
            recv_sem=recv_sems.at[stage],
            device_id=(ring, to),
            device_id_type=MESH,
        ).start()

    def drain(stage, sent, got):
        if sent is not None:
            pltpu.make_async_copy(sent, sent, send_sems.at[stage]).wait()
        if got is not None:
            pltpu.make_async_copy(got, got, recv_sems.at[stage]).wait()

    def send_half(stage, sent_ref, got_ref, q):
        def step(k, carry):
            to = other(k)
            send(stage, sent_ref.at[q, to], got_ref.at[q, :, mine(held), :], to)
            return carry

        lax.fori_loop(1, peers, step, 0)
        got_ref[q, :, mine(held), :] = sent_ref[q, me]

    others = (peers - 1) * held

    loads[0].wait()
    turn(gin, sent_g, 0)
    pl.semaphore_wait(barrier, peers + rings - 2)

    eight = h_ref.shape[0]

    def send_taps(k, carry):
        to = other(k)
        send(0, h_ref, taps.at[mine(eight), :], to)
        return carry

    lax.fori_loop(1, peers, send_taps, 0)
    send_half(1, sent_g, got_g, 0)
    taps[mine(eight), :] = h_ref[...]
    loads[1].wait()
    turn(gin, sent_g, 1)
    loads[2].wait()
    turn(xin, sent_x, 0)
    loads[3].wait()
    turn(xin, sent_x, 1)
    pad = got_g.shape[2] - blocks * group
    got_g[:, :, blocks * group :, :] = jnp.zeros((2, 2, pad, LANES), got_g.dtype)

    def send_rows(q):
        def step(k, carry):
            to = other(k)
            at = pl.multiple_of(to * held, held)
            send(5 + q, y_rows.at[q, :, pl.ds(at, held), :], got_y.at[q, me], to)
            return carry

        lax.fori_loop(1, peers, step, 0)
        got_y[q, me] = y_rows[q, :, mine(held), :]

    def finish_rows(q):
        drain(5 + q, None, got_y.at[q, 0 : peers - 1])

        def step(k, carry):
            start = pl.multiple_of(k * group, group)
            for side in range(2):
                rows = got_y[q, :, side, pl.ds(start, group), :].reshape(BLK, LANES)
                at = pl.multiple_of(k * BLK + side * LANES, LANES)
                yout[pl.ds(at, LANES), q * BLK : (q + 1) * BLK] = jnp.transpose(rows)
            return carry

        lax.fori_loop(0, near, step, 0)
        cols = early if q == 0 else late
        copy = pltpu.make_async_copy(yout.at[:, cols], y_hbm.at[:, cols], local_sems.at[4 + q])
        copy.start()
        return copy

    drain(0, None, taps.at[0 : (peers - 1) * eight, :])
    build_strip(taps, turned, strip)
    send_half(2, sent_g, got_g, 1)

    drain(1, None, got_g.at[0, :, 0:others, :])
    conv_half(
        got_g, strip, acc, y_rows, 0, blocks, group, lambda: send_half(3, sent_x, got_x, 0)
    )
    drain(2, None, got_g.at[1, :, 0:others, :])
    conv_half(
        got_g, strip, acc, y_rows, 1, blocks, group, lambda: send_half(4, sent_x, got_x, 1)
    )
    send_rows(0)

    def after(span):
        if span == min(1, blocks * group // BLK - 1):
            send_rows(1)

    drain(3, None, got_x.at[0, :, 0:others, :])
    turn_inputs(got_x, xt, 0)
    corr_first(got_g, xt, cross_sums, blocks, group, after)
    drain(4, None, got_x.at[1, :, 0:others, :])
    turn_inputs(got_x, xt, 1)
    corr_last(got_g, xt, cross_sums, part, lag, blocks, group)

    def send_lags(k, carry):
        to = other(k)
        source = lag.at[pl.ds(pl.multiple_of(to * eight, eight), eight), :]
        send(7, source, got_lag.at[me], to)
        return carry

    lax.fori_loop(1, peers, send_lags, 0)
    got_lag[me] = lag[mine(eight), :]

    stores = [finish_rows(0), finish_rows(1)]
    drain(7, None, got_lag.at[0 : peers - 1])
    lag_mine[...] = jnp.sum(got_lag[...], axis=0)

    def send_ring(k, carry):
        to = lax.rem(ring + k, rings)
        pltpu.make_async_remote_copy(
            src_ref=lag_mine,
            dst_ref=got_ring.at[ring],
            send_sem=send_sems.at[8],
            recv_sem=recv_sems.at[8],
            device_id=(to, me),
            device_id_type=MESH,
        ).start()
        return carry

    lax.fori_loop(1, rings, send_ring, 0)
    got_ring[ring] = lag_mine[...]

    drain(0, taps.at[0 : (peers - 1) * eight, :], None)
    for q in range(2):
        drain(1 + q, sent_g.at[q, 0 : peers - 1], None)
        drain(3 + q, sent_x.at[q, 0 : peers - 1], None)
        drain(5 + q, y_rows.at[q, :, 0:others, :], None)
    drain(7, lag.at[0 : (peers - 1) * eight, :], None)
    if rings > 1:
        drain(8, got_ring.at[0 : rings - 1], got_ring.at[0 : rings - 1])
    lag_out[...] = jnp.sum(got_ring[...], axis=0)
    for store in stores:
        store.wait()


def on_device(inputs, grad_out, conv_filter):
    peers = lax.axis_size("seq")
    rings = lax.axis_size("dp")
    local, channels = inputs.shape[1:]
    taps = local * peers
    blocks = taps // BLK
    group = channels // 2 // peers
    near = local // BLK
    rows = blocks * group
    held = near * group
    eight = local // LANES
    half = jnp.bfloat16
    whole = jnp.float32
    anywhere = pl.BlockSpec(memory_space=pl.ANY)
    inside = pl.BlockSpec(memory_space=pltpu.VMEM)
    y, lags = pl.pallas_call(
        functools.partial(kernel, peers, rings),
        in_specs=[anywhere, anywhere, inside],
        out_specs=[anywhere, inside],
        out_shape=[
            jax.ShapeDtypeStruct((local, channels), half),
            jax.ShapeDtypeStruct((eight, LANES), whole),
        ],
        scratch_shapes=[
            pltpu.VMEM((local, channels), half),
            pltpu.VMEM((local, channels), half),
            pltpu.VMEM((2, peers, 2, held, LANES), half),
            pltpu.VMEM((2, peers, 2, held, LANES), half),
            pltpu.VMEM((taps // LANES, LANES), half),
            pltpu.VMEM((taps // LANES, LANES), whole),
            pltpu.VMEM((taps + LANES, LANES), half),
            pltpu.VMEM((2, 2, rows + BLK, LANES), half),
            pltpu.VMEM((2, 2, rows, LANES), half),
            pltpu.VMEM((rows // LANES, BLK, LANES), half),
            pltpu.VMEM((TILE * group, BLK), whole),
            pltpu.VMEM((blocks, BLK, BLK), whole),
            pltpu.VMEM((2 * blocks, 8, LANES), whole),
            pltpu.VMEM((2 * blocks, LANES), whole),
            pltpu.VMEM((2, 2, rows, LANES), half),
            pltpu.VMEM((2, peers, 2, held, LANES), half),
            pltpu.VMEM((local, channels), half),
            pltpu.VMEM((peers, eight, LANES), whole),
            pltpu.VMEM((eight, LANES), whole),
            pltpu.VMEM((rings, eight, LANES), whole),
            pltpu.SemaphoreType.DMA((9,)),
            pltpu.SemaphoreType.DMA((9,)),
            pltpu.SemaphoreType.DMA((6,)),
        ],
        compiler_params=pltpu.CompilerParams(
            collective_id=0, has_side_effects=True, vmem_limit_bytes=56 << 20
        ),
        name="hyena_backward",
    )(inputs[0], grad_out[0], conv_filter.reshape(eight, LANES))
    return y[None], lags.reshape(local)


def solution(mesh):
    placed = (P("dp", "seq", None), P("dp", "seq", None), P("seq"))
    return jax.shard_map(
        on_device,
        mesh=mesh,
        in_specs=placed,
        out_specs=(P("dp", "seq", None), P("seq")),
        check_vma=False,
    )
```

```python
import functools

import jax
import jax.numpy as jnp
from jax import lax
from jax.experimental import pallas as pl
from jax.experimental.pallas import tpu as pltpu
from jax.sharding import PartitionSpec as P

BLK = 256
LANES = 128
DEEP = 16
TILE = 16
NT = (((1,), (1,)), ((), ()))
MESH = pl.DeviceIdType.MESH


def dot(a, b):
    return jnp.dot(a, b, preferred_element_type=jnp.float32)


def flip_matrix(size, dtype):
    row = lax.broadcasted_iota(jnp.int32, (size, size), 0)
    col = lax.broadcasted_iota(jnp.int32, (size, size), 1)
    return jnp.where(row + col == size - 1, 1.0, 0.0).astype(dtype)


def spread(tile):
    return pltpu.roll(tile, 1, 1, stride=1, stride_axis=0)


def lower_mask():
    row = lax.broadcasted_iota(jnp.int32, (LANES, LANES), 0)
    lane = lax.broadcasted_iota(jnp.int32, (LANES, LANES), 1)
    return lane <= row


def build_strip(taps_ref, turned_ref, strip_ref):
    count = taps_ref.shape[0]
    unroll = 8
    turned_ref[...] = dot(taps_ref[...], flip_matrix(LANES, taps_ref.dtype))
    keep = lower_mask()
    zero = jnp.zeros((LANES, LANES), jnp.float32)
    strip_ref[0:LANES, :] = zero.astype(strip_ref.dtype)

    def step(k, before):
        for u in range(unroll):
            q = k * unroll + u
            here = spread(jnp.broadcast_to(turned_ref[pl.ds(q, 1), :], (LANES, LANES)))
            at = pl.multiple_of((q + 1) * LANES, LANES)
            strip_ref[pl.ds(at, LANES), :] = jnp.where(keep, here, before).astype(strip_ref.dtype)
            before = here
        return before

    lax.fori_loop(0, count // unroll, step, zero)


def toeplitz(strip_ref, first, count):
    at = pl.multiple_of(first * BLK, BLK)
    near = strip_ref[pl.ds(at + LANES, count * BLK), :]
    far = strip_ref[pl.ds(at, count * BLK), :]
    return jnp.concatenate([near, far], axis=1)


def conv_half(g_ref, strip_ref, acc_ref, y_ref, q, blocks, group, after):
    rows = TILE * group
    half = TILE // 2
    count = blocks // TILE

    def tile(t, carry):
        row = t * TILE
        left = blocks - row - TILE
        acc_ref[...] = jnp.zeros_like(acc_ref)

        def piece(d, width, height):
            parts = []
            for u in range(width):
                at = pl.multiple_of((row + d + u) * group, group)
                parts += [g_ref[q, 0, pl.ds(at, height), :], g_ref[q, 1, pl.ds(at, height), :]]
            return dot(jnp.concatenate(parts, axis=1), toeplitz(strip_ref, d, width))

        def main(k, carry):
            acc_ref[...] += piece(k * TILE, TILE, rows)
            return carry

        lax.fori_loop(0, count - 1 - t, main, 0)
        acc_ref[...] += piece(left, half, rows)
        acc_ref[0 : rows // 2, :] += piece(left + half, half, rows // 2)
        done = acc_ref[...].astype(y_ref.dtype)
        at = pl.multiple_of(t * rows, rows)
        y_ref[q, 0, pl.ds(at, rows), :] = done[:, 0:LANES]
        y_ref[q, 1, pl.ds(at, rows), :] = done[:, LANES:]
        pl.when(t == 0)(after)
        return carry

    lax.fori_loop(0, count, tile, 0)


def turn_inputs(x_ref, xt_ref, q):
    flip = flip_matrix(BLK, x_ref.dtype)

    def step(k, carry):
        at = pl.multiple_of(k * BLK, BLK)
        block = jnp.concatenate(
            [x_ref[q, 0, pl.ds(at, BLK), :], x_ref[q, 1, pl.ds(at, BLK), :]], axis=1
        )
        turned = lax.dot_general(flip, block, NT, preferred_element_type=jnp.float32)
        turned = turned.astype(xt_ref.dtype)
        xt_ref[2 * k] = turned[:, 0:LANES]
        xt_ref[2 * k + 1] = turned[:, LANES:]
        return carry

    lax.fori_loop(0, x_ref.shape[2] // BLK, step, 0)


def cross(g_ref, xt_ref, q, d, depth, group):
    at = pl.multiple_of(d * group, group)
    left = jnp.concatenate([xt_ref[k] for k in range(depth // LANES)], axis=1)
    right = jnp.concatenate(
        [g_ref[q, 0, pl.ds(at, depth), :], g_ref[q, 1, pl.ds(at, depth), :]], axis=1
    )
    return dot(left, right)


def corr_first(g_ref, xt_ref, cross_ref, blocks, group, after):
    each = BLK // group
    for span in range(blocks // each):
        depth = blocks * group - span * BLK

        def step(k, carry):
            for u in range(DEEP):
                d = span * each + DEEP * k + u
                cross_ref[d] = cross(g_ref, xt_ref, 0, d, depth, group)
            return carry

        lax.fori_loop(0, each // DEEP, step, 0)
        after(span)


def corr_last(g_ref, xt_ref, cross_ref, part_ref, lag_ref, blocks, group):
    each = BLK // group
    keep = lower_mask()
    zero = jnp.zeros((LANES, LANES), jnp.float32)

    def tile_sum(low, high):
        picked = jnp.where(keep, low, high)
        return jnp.sum(picked.reshape(LANES // 8, 8, LANES), axis=0)

    carry = (zero, zero)
    for span in range(blocks // each):
        depth = blocks * group - span * BLK

        def step(k, carry):
            even, half = carry
            for u in range(DEEP):
                d = span * each + DEEP * k + u
                c = cross_ref[d] + cross(g_ref, xt_ref, 1, d, depth, group)
                odd = spread(half + c[0:LANES, 0:LANES])
                here = spread(c[LANES:, 0:LANES] + c[0:LANES, LANES:])
                part_ref[jnp.maximum(2 * d - 2, 0)] = tile_sum(even, odd)
                part_ref[jnp.maximum(2 * d - 1, 0)] = tile_sum(odd, here)
                even, half = here, c[LANES:, LANES:]
            return even, half

        carry = lax.fori_loop(0, each // DEEP, step, carry)
    even, half = carry
    odd = spread(half)
    part_ref[2 * blocks - 2] = tile_sum(even, odd)
    part_ref[2 * blocks - 1] = tile_sum(odd, zero)
    lag_ref[...] = jnp.sum(part_ref[...], axis=1)


def kernel(
    peers,
    rings,
    x_hbm,
    g_hbm,
    h_ref,
    yout,
    lag_out,
    gin,
    xin,
    sent_g,
    sent_x,
    taps,
    turned,
    strip,
    got_g,
    got_x,
    xt,
    acc,
    cross_sums,
    part,
    lag,
    y_rows,
    got_y,
    got_lag,
    lag_mine,
    got_ring,
    send_sems,
    recv_sems,
    local_sems,
):
    me = lax.axis_index("seq")
    ring = lax.axis_index("dp")
    local, channels = gin.shape
    near = local // BLK
    blocks = near * peers
    group = channels // 2 // peers
    held = near * group

    def other(k):
        return lax.rem(me + k, peers)

    def load(k, source, target, cols):
        copy = pltpu.make_async_copy(source.at[:, cols], target.at[:, cols], local_sems.at[k])
        copy.start()
        return copy

    early, late = pl.ds(0, BLK), pl.ds(BLK, BLK)
    loads = [
        load(0, g_hbm, gin, early),
        load(1, g_hbm, gin, late),
        load(2, x_hbm, xin, early),
        load(3, x_hbm, xin, late),
    ]

    barrier = pltpu.get_barrier_semaphore()

    def greet(k, carry):
        pl.semaphore_signal(barrier, inc=1, device_id=(ring, other(k)), device_id_type=MESH)
        return carry

    def greet_ring(k, carry):
        to = lax.rem(ring + k, rings)
        pl.semaphore_signal(barrier, inc=1, device_id=(to, me), device_id_type=MESH)
        return carry

    lax.fori_loop(1, peers, greet, 0)
    lax.fori_loop(1, rings, greet_ring, 0)

    def turn(in_ref, sent_ref, q):
        def step(k, carry):
            at = pl.multiple_of(k * BLK, BLK)
            to = pl.multiple_of(k * group, group)
            block = jnp.transpose(in_ref[pl.ds(at, BLK), q * BLK : (q + 1) * BLK])
            for p in range(peers):
                for side in range(2):
                    sent_ref[q, p, side, pl.ds(to, group), :] = block[
                        p * group : (p + 1) * group, side * LANES : (side + 1) * LANES
                    ]
            return carry

        lax.fori_loop(0, near, step, 0)

    def mine(rows):
        return pl.ds(pl.multiple_of(me * rows, rows), rows)

    def send(stage, source, target, to):
        pltpu.make_async_remote_copy(
            src_ref=source,
            dst_ref=target,
            send_sem=send_sems.at[stage],
            recv_sem=recv_sems.at[stage],
            device_id=(ring, to),
            device_id_type=MESH,
        ).start()

    def drain(stage, sent, got):
        if sent is not None:
            pltpu.make_async_copy(sent, sent, send_sems.at[stage]).wait()
        if got is not None:
            pltpu.make_async_copy(got, got, recv_sems.at[stage]).wait()

    def send_half(stage, sent_ref, got_ref, q):
        def step(k, carry):
            to = other(k)
            send(stage, sent_ref.at[q, to], got_ref.at[q, :, mine(held), :], to)
            return carry

        lax.fori_loop(1, peers, step, 0)
        got_ref[q, :, mine(held), :] = sent_ref[q, me]

    others = (peers - 1) * held

    loads[0].wait()
    turn(gin, sent_g, 0)
    pl.semaphore_wait(barrier, peers + rings - 2)

    eight = h_ref.shape[0]

    def send_taps(k, carry):
        to = other(k)
        send(0, h_ref, taps.at[mine(eight), :], to)
        return carry

    lax.fori_loop(1, peers, send_taps, 0)
    send_half(1, sent_g, got_g, 0)
    taps[mine(eight), :] = h_ref[...]
    loads[1].wait()
    turn(gin, sent_g, 1)
    loads[2].wait()
    turn(xin, sent_x, 0)
    loads[3].wait()
    turn(xin, sent_x, 1)
    pad = got_g.shape[2] - blocks * group
    got_g[:, :, blocks * group :, :] = jnp.zeros((2, 2, pad, LANES), got_g.dtype)

    def send_rows(q):
        def step(k, carry):
            to = other(k)
            at = pl.multiple_of(to * held, held)
            send(5 + q, y_rows.at[q, :, pl.ds(at, held), :], got_y.at[q, me], to)
            return carry

        lax.fori_loop(1, peers, step, 0)
        got_y[q, me] = y_rows[q, :, mine(held), :]

    def finish_rows(q):
        drain(5 + q, None, got_y.at[q, 0 : peers - 1])

        def step(k, carry):
            start = pl.multiple_of(k * group, group)
            for side in range(2):
                rows = got_y[q, :, side, pl.ds(start, group), :].reshape(BLK, LANES)
                at = pl.multiple_of(k * BLK + side * LANES, LANES)
                yout[pl.ds(at, LANES), q * BLK : (q + 1) * BLK] = jnp.transpose(rows)
            return carry

        lax.fori_loop(0, near, step, 0)

    drain(0, None, taps.at[0 : (peers - 1) * eight, :])
    build_strip(taps, turned, strip)
    send_half(2, sent_g, got_g, 1)

    drain(1, None, got_g.at[0, :, 0:others, :])
    conv_half(
        got_g, strip, acc, y_rows, 0, blocks, group, lambda: send_half(3, sent_x, got_x, 0)
    )
    drain(2, None, got_g.at[1, :, 0:others, :])
    conv_half(
        got_g, strip, acc, y_rows, 1, blocks, group, lambda: send_half(4, sent_x, got_x, 1)
    )
    send_rows(0)

    def after(span):
        if span == min(1, blocks * group // BLK - 1):
            send_rows(1)

    drain(3, None, got_x.at[0, :, 0:others, :])
    turn_inputs(got_x, xt, 0)
    corr_first(got_g, xt, cross_sums, blocks, group, after)
    drain(4, None, got_x.at[1, :, 0:others, :])
    turn_inputs(got_x, xt, 1)
    corr_last(got_g, xt, cross_sums, part, lag, blocks, group)

    def send_lags(k, carry):
        to = other(k)
        source = lag.at[pl.ds(pl.multiple_of(to * eight, eight), eight), :]
        send(7, source, got_lag.at[me], to)
        return carry

    lax.fori_loop(1, peers, send_lags, 0)
    got_lag[me] = lag[mine(eight), :]

    finish_rows(0)
    finish_rows(1)
    drain(7, None, got_lag.at[0 : peers - 1])
    lag_mine[...] = jnp.sum(got_lag[...], axis=0)

    def send_ring(k, carry):
        to = lax.rem(ring + k, rings)
        pltpu.make_async_remote_copy(
            src_ref=lag_mine,
            dst_ref=got_ring.at[ring],
            send_sem=send_sems.at[8],
            recv_sem=recv_sems.at[8],
            device_id=(to, me),
            device_id_type=MESH,
        ).start()
        return carry

    lax.fori_loop(1, rings, send_ring, 0)
    got_ring[ring] = lag_mine[...]

    drain(0, taps.at[0 : (peers - 1) * eight, :], None)
    for q in range(2):
        drain(1 + q, sent_g.at[q, 0 : peers - 1], None)
        drain(3 + q, sent_x.at[q, 0 : peers - 1], None)
        drain(5 + q, y_rows.at[q, :, 0:others, :], None)
    drain(7, lag.at[0 : (peers - 1) * eight, :], None)
    if rings > 1:
        drain(8, got_ring.at[0 : rings - 1], got_ring.at[0 : rings - 1])
    lag_out[...] = jnp.sum(got_ring[...], axis=0)


def on_device(inputs, grad_out, conv_filter):
    peers = lax.axis_size("seq")
    rings = lax.axis_size("dp")
    local, channels = inputs.shape[1:]
    taps = local * peers
    blocks = taps // BLK
    group = channels // 2 // peers
    near = local // BLK
    rows = blocks * group
    held = near * group
    eight = local // LANES
    half = jnp.bfloat16
    whole = jnp.float32
    anywhere = pl.BlockSpec(memory_space=pl.ANY)
    inside = pl.BlockSpec(memory_space=pltpu.VMEM)
    y, lags = pl.pallas_call(
        functools.partial(kernel, peers, rings),
        in_specs=[anywhere, anywhere, inside],
        out_specs=[inside, inside],
        out_shape=[
            pltpu.VMEM((local, channels), half),
            pltpu.VMEM((eight, LANES), whole),
        ],
        scratch_shapes=[
            pltpu.VMEM((local, channels), half),
            pltpu.VMEM((local, channels), half),
            pltpu.VMEM((2, peers, 2, held, LANES), half),
            pltpu.VMEM((2, peers, 2, held, LANES), half),
            pltpu.VMEM((taps // LANES, LANES), half),
            pltpu.VMEM((taps // LANES, LANES), whole),
            pltpu.VMEM((taps + LANES, LANES), half),
            pltpu.VMEM((2, 2, rows + BLK, LANES), half),
            pltpu.VMEM((2, 2, rows, LANES), half),
            pltpu.VMEM((rows // LANES, BLK, LANES), half),
            pltpu.VMEM((TILE * group, BLK), whole),
            pltpu.VMEM((blocks, BLK, BLK), whole),
            pltpu.VMEM((2 * blocks, 8, LANES), whole),
            pltpu.VMEM((2 * blocks, LANES), whole),
            pltpu.VMEM((2, 2, rows, LANES), half),
            pltpu.VMEM((2, peers, 2, held, LANES), half),
            pltpu.VMEM((peers, eight, LANES), whole),
            pltpu.VMEM((eight, LANES), whole),
            pltpu.VMEM((rings, eight, LANES), whole),
            pltpu.SemaphoreType.DMA((9,)),
            pltpu.SemaphoreType.DMA((9,)),
            pltpu.SemaphoreType.DMA((4,)),
        ],
        compiler_params=pltpu.CompilerParams(
            collective_id=0, has_side_effects=True, vmem_limit_bytes=56 << 20
        ),
        name="hyena_backward",
    )(inputs[0], grad_out[0], conv_filter.reshape(eight, LANES))
    return y[None], lags.reshape(local)


def solution(mesh):
    placed = (P("dp", "seq", None), P("dp", "seq", None), P("seq"))
    return jax.shard_map(
        on_device,
        mesh=mesh,
        in_specs=placed,
        out_specs=(P("dp", "seq", None), P("seq")),
        check_vma=False,
    )
```

```python
import functools

import jax
import jax.numpy as jnp
from jax import lax
from jax.experimental import pallas as pl
from jax.experimental.pallas import tpu as pltpu
from jax.sharding import PartitionSpec as P

BLK = 256
LANES = 128
DEEP = 16
TILE = 16
NT = (((1,), (1,)), ((), ()))
MESH = pl.DeviceIdType.MESH


def dot(a, b):
    return jnp.dot(a, b, preferred_element_type=jnp.float32)


def flip_matrix(size, dtype):
    row = lax.broadcasted_iota(jnp.int32, (size, size), 0)
    col = lax.broadcasted_iota(jnp.int32, (size, size), 1)
    return jnp.where(row + col == size - 1, 1.0, 0.0).astype(dtype)


def spread(tile):
    return pltpu.roll(tile, 1, 1, stride=1, stride_axis=0)


def lower_mask():
    row = lax.broadcasted_iota(jnp.int32, (LANES, LANES), 0)
    lane = lax.broadcasted_iota(jnp.int32, (LANES, LANES), 1)
    return lane <= row


def build_strip(taps_ref, turned_ref, strip_ref):
    count = taps_ref.shape[0]
    unroll = 8
    turned_ref[...] = dot(taps_ref[...], flip_matrix(LANES, taps_ref.dtype))
    keep = lower_mask()
    zero = jnp.zeros((LANES, LANES), jnp.float32)
    strip_ref[0:LANES, :] = zero.astype(strip_ref.dtype)

    def step(k, before):
        for u in range(unroll):
            q = k * unroll + u
            here = spread(jnp.broadcast_to(turned_ref[pl.ds(q, 1), :], (LANES, LANES)))
            at = pl.multiple_of((q + 1) * LANES, LANES)
            strip_ref[pl.ds(at, LANES), :] = jnp.where(keep, here, before).astype(strip_ref.dtype)
            before = here
        return before

    lax.fori_loop(0, count // unroll, step, zero)


def toeplitz(strip_ref, first, count):
    at = pl.multiple_of(first * BLK, BLK)
    near = strip_ref[pl.ds(at + LANES, count * BLK), :]
    far = strip_ref[pl.ds(at, count * BLK), :]
    return jnp.concatenate([near, far], axis=1)


def conv_half(g_ref, strip_ref, acc_ref, y_ref, q, blocks, group, after):
    rows = TILE * group
    half = TILE // 2
    count = blocks // TILE

    def tile(t, carry):
        row = t * TILE
        left = blocks - row - TILE
        acc_ref[...] = jnp.zeros_like(acc_ref)

        def piece(d, width, height):
            parts = []
            for u in range(width):
                at = pl.multiple_of((row + d + u) * group, group)
                parts += [g_ref[q, 0, pl.ds(at, height), :], g_ref[q, 1, pl.ds(at, height), :]]
            return dot(jnp.concatenate(parts, axis=1), toeplitz(strip_ref, d, width))

        def main(k, carry):
            acc_ref[...] += piece(k * TILE, TILE, rows)
            return carry

        lax.fori_loop(0, count - 1 - t, main, 0)
        acc_ref[...] += piece(left, half, rows)
        acc_ref[0 : rows // 2, :] += piece(left + half, half, rows // 2)
        done = acc_ref[...].astype(y_ref.dtype)
        at = pl.multiple_of(t * rows, rows)
        y_ref[q, 0, pl.ds(at, rows), :] = done[:, 0:LANES]
        y_ref[q, 1, pl.ds(at, rows), :] = done[:, LANES:]
        pl.when(t == 0)(after)
        return carry

    lax.fori_loop(0, count, tile, 0)


def turn_inputs(x_ref, xt_ref, q):
    flip = flip_matrix(BLK, x_ref.dtype)

    def step(k, carry):
        at = pl.multiple_of(k * BLK, BLK)
        block = jnp.concatenate(
            [x_ref[q, 0, pl.ds(at, BLK), :], x_ref[q, 1, pl.ds(at, BLK), :]], axis=1
        )
        turned = lax.dot_general(flip, block, NT, preferred_element_type=jnp.float32)
        turned = turned.astype(xt_ref.dtype)
        xt_ref[2 * k] = turned[:, 0:LANES]
        xt_ref[2 * k + 1] = turned[:, LANES:]
        return carry

    lax.fori_loop(0, x_ref.shape[2] // BLK, step, 0)


def cross(g_ref, xt_ref, q, d, depth, group):
    at = pl.multiple_of(d * group, group)
    left = jnp.concatenate([xt_ref[k] for k in range(depth // LANES)], axis=1)
    right = jnp.concatenate(
        [g_ref[q, 0, pl.ds(at, depth), :], g_ref[q, 1, pl.ds(at, depth), :]], axis=1
    )
    return dot(left, right)


def corr_first(g_ref, xt_ref, cross_ref, blocks, group, after):
    each = BLK // group
    for span in range(blocks // each):
        depth = blocks * group - span * BLK

        def step(k, carry):
            for u in range(DEEP):
                d = span * each + DEEP * k + u
                cross_ref[d] = cross(g_ref, xt_ref, 0, d, depth, group)
            return carry

        lax.fori_loop(0, each // DEEP, step, 0)
        after(span)


def corr_last(g_ref, xt_ref, cross_ref, part_ref, blocks, group, share, ready):
    each = BLK // group
    keep = lower_mask()
    zero = jnp.zeros((LANES, LANES), jnp.float32)

    def tile_sum(low, high):
        picked = jnp.where(keep, low, high)
        return jnp.sum(picked.reshape(LANES // 8, 8, LANES), axis=0)

    carry = (zero, zero)
    since = 0
    for span in range(blocks // each):
        depth = blocks * group - span * BLK

        def step(k, carry):
            even, half = carry
            for u in range(DEEP):
                d = span * each + DEEP * k + u
                c = cross_ref[d] + cross(g_ref, xt_ref, 1, d, depth, group)
                odd = spread(half + c[0:LANES, 0:LANES])
                here = spread(c[LANES:, 0:LANES] + c[0:LANES, LANES:])
                part_ref[jnp.maximum(2 * d - 2, 0)] = tile_sum(even, odd)
                part_ref[jnp.maximum(2 * d - 1, 0)] = tile_sum(odd, here)
                even, half = here, c[LANES:, LANES:]
            return even, half

        carry = lax.fori_loop(0, each // DEEP, step, carry)
        until = (2 * each * (span + 1) - 2) // share
        ready(since, until)
        since = until
    even, half = carry
    odd = spread(half)
    part_ref[2 * blocks - 2] = tile_sum(even, odd)
    part_ref[2 * blocks - 1] = tile_sum(odd, zero)
    ready(since, 2 * blocks // share)


def kernel(
    peers,
    rings,
    x_hbm,
    g_hbm,
    h_ref,
    yout,
    lag_out,
    gin,
    xin,
    sent_g,
    sent_x,
    taps,
    turned,
    strip,
    got_g,
    got_x,
    xt,
    acc,
    cross_sums,
    part,
    lag,
    y_rows,
    got_y,
    got_lag,
    lag_mine,
    got_ring,
    send_sems,
    recv_sems,
    local_sems,
):
    me = lax.axis_index("seq")
    ring = lax.axis_index("dp")
    local, channels = gin.shape
    near = local // BLK
    blocks = near * peers
    group = channels // 2 // peers
    held = near * group

    def other(k):
        return lax.rem(me + k, peers)

    def load(k, source, target, cols):
        copy = pltpu.make_async_copy(source.at[:, cols], target.at[:, cols], local_sems.at[k])
        copy.start()
        return copy

    early, late = pl.ds(0, BLK), pl.ds(BLK, BLK)
    loads = [
        load(0, g_hbm, gin, early),
        load(1, g_hbm, gin, late),
        load(2, x_hbm, xin, early),
        load(3, x_hbm, xin, late),
    ]

    barrier = pltpu.get_barrier_semaphore()

    def greet(k, carry):
        pl.semaphore_signal(barrier, inc=1, device_id=(ring, other(k)), device_id_type=MESH)
        return carry

    def greet_ring(k, carry):
        to = lax.rem(ring + k, rings)
        pl.semaphore_signal(barrier, inc=1, device_id=(to, me), device_id_type=MESH)
        return carry

    lax.fori_loop(1, peers, greet, 0)
    lax.fori_loop(1, rings, greet_ring, 0)

    def turn(in_ref, sent_ref, q):
        def step(k, carry):
            at = pl.multiple_of(k * BLK, BLK)
            to = pl.multiple_of(k * group, group)
            block = jnp.transpose(in_ref[pl.ds(at, BLK), q * BLK : (q + 1) * BLK])
            for p in range(peers):
                for side in range(2):
                    sent_ref[q, p, side, pl.ds(to, group), :] = block[
                        p * group : (p + 1) * group, side * LANES : (side + 1) * LANES
                    ]
            return carry

        lax.fori_loop(0, near, step, 0)

    def mine(rows):
        return pl.ds(pl.multiple_of(me * rows, rows), rows)

    def send(stage, source, target, to):
        pltpu.make_async_remote_copy(
            src_ref=source,
            dst_ref=target,
            send_sem=send_sems.at[stage],
            recv_sem=recv_sems.at[stage],
            device_id=(ring, to),
            device_id_type=MESH,
        ).start()

    def drain(stage, sent, got):
        if sent is not None:
            pltpu.make_async_copy(sent, sent, send_sems.at[stage]).wait()
        if got is not None:
            pltpu.make_async_copy(got, got, recv_sems.at[stage]).wait()

    def send_half(stage, sent_ref, got_ref, q):
        def step(k, carry):
            to = other(k)
            send(stage, sent_ref.at[q, to], got_ref.at[q, :, mine(held), :], to)
            return carry

        lax.fori_loop(1, peers, step, 0)
        got_ref[q, :, mine(held), :] = sent_ref[q, me]

    others = (peers - 1) * held

    loads[0].wait()
    turn(gin, sent_g, 0)
    pl.semaphore_wait(barrier, peers + rings - 2)

    eight = h_ref.shape[0]

    def send_taps(k, carry):
        to = other(k)
        send(0, h_ref, taps.at[mine(eight), :], to)
        return carry

    lax.fori_loop(1, peers, send_taps, 0)
    send_half(1, sent_g, got_g, 0)
    taps[mine(eight), :] = h_ref[...]
    loads[1].wait()
    turn(gin, sent_g, 1)
    loads[2].wait()
    turn(xin, sent_x, 0)
    loads[3].wait()
    turn(xin, sent_x, 1)
    pad = got_g.shape[2] - blocks * group
    got_g[:, :, blocks * group :, :] = jnp.zeros((2, 2, pad, LANES), got_g.dtype)

    def send_rows(q):
        def step(k, carry):
            to = other(k)
            at = pl.multiple_of(to * held, held)
            send(5 + q, y_rows.at[q, :, pl.ds(at, held), :], got_y.at[q, me], to)
            return carry

        lax.fori_loop(1, peers, step, 0)
        got_y[q, me] = y_rows[q, :, mine(held), :]

    def finish_rows(q):
        drain(5 + q, None, got_y.at[q, 0 : peers - 1])

        def step(k, carry):
            start = pl.multiple_of(k * group, group)
            for side in range(2):
                rows = got_y[q, :, side, pl.ds(start, group), :].reshape(BLK, LANES)
                at = pl.multiple_of(k * BLK + side * LANES, LANES)
                yout[pl.ds(at, LANES), q * BLK : (q + 1) * BLK] = jnp.transpose(rows)
            return carry

        lax.fori_loop(0, near, step, 0)

    drain(0, None, taps.at[0 : (peers - 1) * eight, :])
    build_strip(taps, turned, strip)
    send_half(2, sent_g, got_g, 1)

    drain(1, None, got_g.at[0, :, 0:others, :])
    conv_half(
        got_g, strip, acc, y_rows, 0, blocks, group, lambda: send_half(3, sent_x, got_x, 0)
    )
    drain(2, None, got_g.at[1, :, 0:others, :])
    conv_half(
        got_g, strip, acc, y_rows, 1, blocks, group, lambda: send_half(4, sent_x, got_x, 1)
    )
    send_rows(0)

    def after(span):
        if span == min(1, blocks * group // BLK - 1):
            send_rows(1)

    drain(3, None, got_x.at[0, :, 0:others, :])
    turn_inputs(got_x, xt, 0)
    corr_first(got_g, xt, cross_sums, blocks, group, after)
    drain(4, None, got_x.at[1, :, 0:others, :])
    turn_inputs(got_x, xt, 1)

    def ready(first, last):
        if first == last:
            return
        lag[first * eight : last * eight, :] = jnp.sum(part[first * eight : last * eight], axis=1)

        def step(k, carry):
            p = first + lax.rem(me + k, last - first)

            @pl.when(p != me)
            def _():
                source = lag.at[pl.ds(pl.multiple_of(p * eight, eight), eight), :]
                send(7, source, got_lag.at[me], p)

            return carry

        lax.fori_loop(0, last - first, step, 0)

    corr_last(got_g, xt, cross_sums, part, blocks, group, eight, ready)
    got_lag[me] = lag[mine(eight), :]

    finish_rows(0)
    finish_rows(1)
    drain(7, None, got_lag.at[0 : peers - 1])
    lag_mine[...] = jnp.sum(got_lag[...], axis=0)

    def send_ring(k, carry):
        to = lax.rem(ring + k, rings)
        pltpu.make_async_remote_copy(
            src_ref=lag_mine,
            dst_ref=got_ring.at[ring],
            send_sem=send_sems.at[8],
            recv_sem=recv_sems.at[8],
            device_id=(to, me),
            device_id_type=MESH,
        ).start()
        return carry

    lax.fori_loop(1, rings, send_ring, 0)
    got_ring[ring] = lag_mine[...]

    drain(0, taps.at[0 : (peers - 1) * eight, :], None)
    for q in range(2):
        drain(1 + q, sent_g.at[q, 0 : peers - 1], None)
        drain(3 + q, sent_x.at[q, 0 : peers - 1], None)
        drain(5 + q, y_rows.at[q, :, 0:others, :], None)
    drain(7, lag.at[0 : (peers - 1) * eight, :], None)
    if rings > 1:
        drain(8, got_ring.at[0 : rings - 1], got_ring.at[0 : rings - 1])
    lag_out[...] = jnp.sum(got_ring[...], axis=0)


def on_device(inputs, grad_out, conv_filter):
    peers = lax.axis_size("seq")
    rings = lax.axis_size("dp")
    local, channels = inputs.shape[1:]
    taps = local * peers
    blocks = taps // BLK
    group = channels // 2 // peers
    near = local // BLK
    rows = blocks * group
    held = near * group
    eight = local // LANES
    half = jnp.bfloat16
    whole = jnp.float32
    anywhere = pl.BlockSpec(memory_space=pl.ANY)
    inside = pl.BlockSpec(memory_space=pltpu.VMEM)
    y, lags = pl.pallas_call(
        functools.partial(kernel, peers, rings),
        in_specs=[anywhere, anywhere, inside],
        out_specs=[inside, inside],
        out_shape=[
            pltpu.VMEM((local, channels), half),
            pltpu.VMEM((eight, LANES), whole),
        ],
        scratch_shapes=[
            pltpu.VMEM((local, channels), half),
            pltpu.VMEM((local, channels), half),
            pltpu.VMEM((2, peers, 2, held, LANES), half),
            pltpu.VMEM((2, peers, 2, held, LANES), half),
            pltpu.VMEM((taps // LANES, LANES), half),
            pltpu.VMEM((taps // LANES, LANES), whole),
            pltpu.VMEM((taps + LANES, LANES), half),
            pltpu.VMEM((2, 2, rows + BLK, LANES), half),
            pltpu.VMEM((2, 2, rows, LANES), half),
            pltpu.VMEM((rows // LANES, BLK, LANES), half),
            pltpu.VMEM((TILE * group, BLK), whole),
            pltpu.VMEM((blocks, BLK, BLK), whole),
            pltpu.VMEM((2 * blocks, 8, LANES), whole),
            pltpu.VMEM((2 * blocks, LANES), whole),
            pltpu.VMEM((2, 2, rows, LANES), half),
            pltpu.VMEM((2, peers, 2, held, LANES), half),
            pltpu.VMEM((peers, eight, LANES), whole),
            pltpu.VMEM((eight, LANES), whole),
            pltpu.VMEM((rings, eight, LANES), whole),
            pltpu.SemaphoreType.DMA((9,)),
            pltpu.SemaphoreType.DMA((9,)),
            pltpu.SemaphoreType.DMA((4,)),
        ],
        compiler_params=pltpu.CompilerParams(
            collective_id=0, has_side_effects=True, vmem_limit_bytes=56 << 20
        ),
        name="hyena_backward",
    )(inputs[0], grad_out[0], conv_filter.reshape(eight, LANES))
    return y[None], lags.reshape(local)


def solution(mesh):
    placed = (P("dp", "seq", None), P("dp", "seq", None), P("seq"))
    return jax.shard_map(
        on_device,
        mesh=mesh,
        in_specs=placed,
        out_specs=(P("dp", "seq", None), P("seq")),
        check_vma=False,
    )
```
